128 devices in a mesh: rows: 32 (over x, z, core), cols: 4 (over y).
Axes of the slice: x: 4, y: 4, z: 4, core: 2. Of those that a mesh axis runs over, the one named last changes fastest.
Arguments:
- basis: float32 [262144, 256], P(('rows', 'cols')), may hold values from -8 to 8, as said below
- new_vectors: float32 [262144, 128], P(('rows', 'cols')), may hold values from -180 to 180
- jacobian: float32 [262144, 1024], P(('rows', 'cols')), may hold values from -0.1875 to 0.1875
Outputs:
- merged: float32 [262144, 384], P(('rows', 'cols'))
The draws below stay inside these ranges and needn't reach their ends.
Inputs may be any that keep to these rules, and one draw needn't show every extreme that they name: The stored basis is orthonormal under the inner product divided by 262144 up to a drift of orthogonality: basis^T basis / 262144 differs from the identity by about 0.1 to 0.3 in spectral norm.
All inputs are finite; a program needn't handle non-finite values.
Results may differ from the reference program's by a relative error of at most 0.00005.
Values sent between devices are 32-bit elements; how exact they have to be, the bound alone decides.
A program may use at most 64 MiB of HBM per device.

```python
import math
import jax
import jax.numpy as jnp
from jax import lax

K = 256
B = 128
OBS = 1024
NT = 262144


def draw_basis(key, part):
    raw_key = jax.random.fold_in(key, 5)
    drift_key = jax.random.fold_in(key, 7)
    raw = jax.random.normal(raw_key, (NT, K), jnp.float32)
    gram = lax.dot_general(raw, raw, (((0,), (0,)), ((), ())), precision=lax.Precision.HIGHEST, preferred_element_type=jnp.float32) / NT
    lower = jnp.linalg.cholesky(gram)
    ident = jnp.eye(K, dtype=jnp.float32)
    inverse = lax.linalg.triangular_solve(lower, ident, left_side=True, lower=True)
    ortho = jnp.dot(raw, inverse.T, precision=lax.Precision.HIGHEST, preferred_element_type=jnp.float32)
    drift = jax.random.normal(drift_key, (K, K), jnp.float32) * (0.05 / math.sqrt(K))
    mixed = jnp.dot(ortho, ident + drift, precision=lax.Precision.HIGHEST, preferred_element_type=jnp.float32)
    return jnp.clip(mixed, -8.0, 8.0)


def draw_new_vectors(key, part):
    first_key = jax.random.fold_in(key, 11)
    second_key = jax.random.fold_in(key, 23)
    positions = jnp.arange(NT, dtype=jnp.float32)
    factor = 1.0 + 2.0 * positions / max(NT - 1, 1)
    base = jax.random.normal(first_key, (NT, B), jnp.float32)
    scales = jnp.exp(jax.random.uniform(second_key, (1, B), jnp.float32, 0.0, math.log(10.0)))
    return jnp.clip(base * scales * factor[:, None], -180.0, 180.0)


def block_levels(key, shape, pieces, low, top_value):
    def one(position, shards_of):
        heights = jax.random.uniform(jax.random.fold_in(jax.random.fold_in(key, 6), position), (shards_of,), jnp.float32, low / len(pieces), top_value / len(pieces))
        return jnp.repeat(jnp.exp(heights), shape[position] // shards_of).reshape((-1,) + (1,) * (len(shape) - position - 1))

    factor_of = one(*pieces[0])
    for cut in pieces[1:]:
        factor_of = factor_of * one(*cut)
    return factor_of


def centred(rng, shape, width, limit, shards=(), kind=jnp.bfloat16):
    entries = width * jax.random.normal(rng, shape, jnp.float32)
    if shards:
        entries = entries * block_levels(rng, shape, shards, -0.22, 0.18)
    return jnp.clip(entries, -limit, limit).astype(kind)


def setup_inputs(seed: int = 0) -> dict:
    keys = jax.random.split(jax.random.key(seed), 4)
    basis = draw_basis(jax.random.fold_in(keys[3], 71), 0)
    new_vectors = draw_new_vectors(jax.random.fold_in(keys[3], 71), 0)
    jacobian = centred(keys[2], (NT, OBS), OBS ** -0.5, 0.1875, ((0, 128),), jnp.float32)
    return {"basis": basis, "new_vectors": new_vectors, "jacobian": jacobian}


def mat(left, right):
    return jnp.dot(left.astype(jnp.float32), right.astype(jnp.float32), precision=lax.Precision.HIGHEST, preferred_element_type=jnp.float32)

def tmat(left, right):
    return lax.dot_general(left.astype(jnp.float32), right.astype(jnp.float32), (((0,), (0,)), ((), ())), precision=lax.Precision.HIGHEST, preferred_element_type=jnp.float32)

def inverse_lower(gram):
    lower = jnp.linalg.cholesky(gram)
    ident = jnp.eye(gram.shape[0], dtype=jnp.float32)
    return lax.linalg.triangular_solve(lower, ident, left_side=True, lower=True)

def reference(basis, new_vectors, jacobian):
    scale = 1.0 / NT
    root = 1.0 / jnp.sqrt(jnp.float32(NT))
    first = tmat(basis, new_vectors) * scale
    once = new_vectors - mat(basis, first)
    second = tmat(basis, once) * scale
    cleaned = once - mat(basis, second)
    gram = tmat(cleaned, cleaned) * scale
    fresh = mat(cleaned, inverse_lower(gram).T)
    joined = jnp.concatenate([basis, fresh], axis=1)
    proj = tmat(jacobian, joined) * root
    hess = tmat(proj, proj)
    ident = jnp.eye(hess.shape[0], dtype=jnp.float32)
    outer = inverse_lower(ident + hess)
    return mat(joined, outer.T)
```

```python
import jax
import jax.numpy as jnp
from jax import lax
from jax.sharding import PartitionSpec as P


def mat(left, right, precision=lax.Precision.HIGHEST):
    return jnp.dot(left, right, precision=precision, preferred_element_type=jnp.float32)


def tmat(left, right, precision=lax.Precision.HIGHEST):
    return lax.dot_general(
        left,
        right,
        (((0,), (0,)), ((), ())),
        precision=precision,
        preferred_element_type=jnp.float32,
    )


def inverse_lower(gram):
    lower = jnp.linalg.cholesky(gram)
    ident = jnp.eye(gram.shape[0], dtype=jnp.float32)
    return lax.linalg.triangular_solve(lower, ident, left_side=True, lower=True)


def combine(full, hess, width):
    s_vv = full[:width, :width]
    s_vw = full[:width, width:]
    s_ww = full[width:, width:]
    summed = s_vw + (s_vw - mat(s_vv, s_vw))
    cross = tmat(summed, s_vw)
    gram = s_ww - cross - cross.T + tmat(summed, mat(s_vv, summed))
    ident = jnp.eye(width, dtype=jnp.float32)
    top = jnp.concatenate([ident, summed], axis=1)
    low = jnp.concatenate([summed.T, gram + tmat(summed, summed)], axis=1)
    return jnp.concatenate([top, low], axis=0) + hess


def local(basis, new_vectors, jacobian):
    total = basis.shape[0] * lax.axis_size("rows") * lax.axis_size("cols")
    scale = 1.0 / total
    width = basis.shape[1]
    stacked = jnp.concatenate([basis, new_vectors], axis=1)
    full = tmat(stacked, stacked, lax.Precision.HIGH)
    proj = tmat(jacobian, stacked, lax.Precision.HIGH)
    full, proj = lax.psum((full, proj), ("rows", "cols"))
    hess = tmat(proj, proj) * scale
    inverse = inverse_lower(combine(full * scale, hess, width))
    return lax.dot_general(
        stacked,
        inverse,
        (((1,), (1,)), ((), ())),
        precision=lax.Precision.HIGH,
        preferred_element_type=jnp.float32,
    )


def solution(mesh):
    placed = (P(("rows", "cols"), None), P(("rows", "cols"), None), P(("rows", "cols"), None))
    return jax.shard_map(
        local, mesh=mesh, in_specs=placed, out_specs=P(("rows", "cols"), None), check_vma=False
    )
```

```python
import jax
import jax.numpy as jnp
from jax import lax
from jax.experimental import pallas as pl
from jax.experimental.pallas import tpu as pltpu
from jax.sharding import PartitionSpec as P

SIDE = 4
STREAMS = 4
ORDERS = ((0, 1, 2), (1, 2, 0), (2, 0, 1), (0, 2, 1))
OFFSETS = (2, 1, 3)
ROWS = 1024


def sum_kernel(y_ref, out_ref, z0, r0, z1, r1, z2, r2, r3, s0, t0, s1, t1):
    row, col = lax.axis_index("rows"), lax.axis_index("cols")
    core = lax.rem(row, 2)
    place = (lax.div(row, 2 * SIDE), col, lax.rem(lax.div(row, 2), SIDE))

    def device(coords, which):
        return (coords[0] * (2 * SIDE) + coords[2] * 2 + which, coords[1])

    def peer(axis, offset):
        coords = list(place)
        coords[axis] = lax.rem(place[axis] + offset, SIDE)
        return coords

    partner = device(place, 1 - core)
    barrier = pltpu.get_barrier_semaphore()
    pl.semaphore_signal(barrier, inc=1, device_id=partner, device_id_type=pl.DeviceIdType.MESH)
    for axis in range(3):
        for offset in OFFSETS:
            pl.semaphore_signal(
                barrier, inc=1, device_id=device(peer(axis, offset), core), device_id_type=pl.DeviceIdType.MESH
            )
    pl.semaphore_wait(barrier, 1 + 3 * len(OFFSETS))

    sent = []

    def send(src, dst, send_sem, recv_sem, target):
        copy = pltpu.make_async_remote_copy(
            src_ref=src,
            dst_ref=dst,
            send_sem=send_sem,
            recv_sem=recv_sem,
            device_id=target,
            device_id_type=pl.DeviceIdType.MESH,
        )
        copy.start()
        sent.append(copy)
        return copy

    half = ROWS // 2
    order = (3, 0, 1, 2)
    mine = pl.multiple_of(core * half, half)
    other = pl.multiple_of((1 - core) * half, half)
    stage = {}
    for s in order:
        stage[s] = send(y_ref.at[s, pl.ds(other, half)], r0.at[s], s0.at[0, s], t0.at[0, s], partner)

    size = half
    parts = (r1, r2, r3)
    for phase in range(3):
        size //= SIDE
        nxt = {}
        for s in order:
            axis = ORDERS[s][phase]
            if phase == 0:
                stage[s].wait_recv()
                z0[s] = y_ref[s, pl.ds(mine, half)] + r0[s]
            else:
                for copy in stage[s]:
                    copy.wait_recv()
                before = ORDERS[s][phase - 1]
                prev, got = (z0, r1) if phase == 1 else (z1, r2)
                start = pl.multiple_of(place[before] * (size * SIDE), size * SIDE)
                dest = z1 if phase == 1 else z2
                dest[s] = prev[s, pl.ds(start, size * SIDE)] + got[s, 0] + got[s, 1] + got[s, 2]
            src = (z0, z1, z2)[phase]
            nxt[s] = []
            for slot, offset in enumerate(OFFSETS):
                coords = peer(axis, offset)
                start = pl.multiple_of(coords[axis] * size, size)
                nxt[s].append(
                    send(
                        src.at[s, pl.ds(start, size)],
                        parts[phase].at[s, slot],
                        s1.at[phase, s, slot],
                        t1.at[phase, s, slot],
                        device(coords, core),
                    )
                )
        stage = nxt

    for phase in range(3):
        back = 2 - phase
        nxt = {}
        for s in order:
            axis = ORDERS[s][back]
            for copy in stage[s]:
                copy.wait_recv()
            start = mine
            width = half
            for done in range(back + 1):
                width //= SIDE
                start = start + place[ORDERS[s][done]] * width
            start = pl.multiple_of(start, width)
            if phase == 0:
                own = pl.multiple_of(place[axis] * width, width)
                out_ref[s, pl.ds(start, width)] = z2[s, pl.ds(own, width)] + r3[s, 0] + r3[s, 1] + r3[s, 2]
            nxt[s] = []
            for slot, offset in enumerate(OFFSETS):
                nxt[s].append(
                    send(
                        out_ref.at[s, pl.ds(start, width)],
                        out_ref.at[s, pl.ds(start, width)],
                        s1.at[3 + phase, s, slot],
                        t1.at[3 + phase, s, slot],
                        device(peer(axis, offset), core),
                    )
                )
        stage = nxt
    last = []
    for s in order:
        for copy in stage[s]:
            copy.wait_recv()
        last.append(send(out_ref.at[s, pl.ds(mine, half)], out_ref.at[s, pl.ds(mine, half)], s0.at[1, s], t0.at[1, s], partner))
    for copy in last:
        copy.wait_recv()
    for copy in sent:
        copy.wait_send()


def sum_all(y):
    dma = pltpu.SemaphoreType.DMA
    half = ROWS // 2
    f32 = jnp.float32
    return pl.pallas_call(
        sum_kernel,
        out_shape=jax.ShapeDtypeStruct(y.shape, f32),
        in_specs=[pl.BlockSpec(memory_space=pltpu.VMEM)],
        out_specs=pl.BlockSpec(memory_space=pltpu.VMEM),
        scratch_shapes=[
            pltpu.VMEM((STREAMS, half, 128), f32),
            pltpu.VMEM((STREAMS, half, 128), f32),
            pltpu.VMEM((STREAMS, half // 4, 128), f32),
            pltpu.VMEM((STREAMS, 3, half // 4, 128), f32),
            pltpu.VMEM((STREAMS, half // 16, 128), f32),
            pltpu.VMEM((STREAMS, 3, half // 16, 128), f32),
            pltpu.VMEM((STREAMS, 3, half // 64, 128), f32),
            dma((2, STREAMS)),
            dma((2, STREAMS)),
            dma((6, STREAMS, 3)),
            dma((6, STREAMS, 3)),
        ],
        compiler_params=pltpu.CompilerParams(collective_id=0, has_side_effects=True, vmem_limit_bytes=20 * 1024 * 1024),
        name="sum_all",
    )(y)


def mat(left, right, precision=lax.Precision.HIGHEST):
    return jnp.dot(left, right, precision=precision, preferred_element_type=jnp.float32)


def tmat(left, right, precision=lax.Precision.HIGHEST):
    return lax.dot_general(
        left,
        right,
        (((0,), (0,)), ((), ())),
        precision=precision,
        preferred_element_type=jnp.float32,
    )


def inverse_lower(gram):
    lower = jnp.linalg.cholesky(gram)
    ident = jnp.eye(gram.shape[0], dtype=jnp.float32)
    return lax.linalg.triangular_solve(lower, ident, left_side=True, lower=True)


def combine(full, hess, width):
    s_vv = full[:width, :width]
    s_vw = full[:width, width:]
    s_ww = full[width:, width:]
    summed = s_vw + (s_vw - mat(s_vv, s_vw))
    cross = tmat(summed, s_vw)
    gram = s_ww - cross - cross.T + tmat(summed, mat(s_vv, summed))
    ident = jnp.eye(width, dtype=jnp.float32)
    top = jnp.concatenate([ident, summed], axis=1)
    low = jnp.concatenate([summed.T, gram + tmat(summed, summed)], axis=1)
    return jnp.concatenate([top, low], axis=0) + hess


def local(basis, new_vectors, jacobian):
    total = basis.shape[0] * lax.axis_size("rows") * lax.axis_size("cols")
    scale = 1.0 / total
    width = basis.shape[1]
    stacked = jnp.concatenate([basis, new_vectors], axis=1)
    full = tmat(stacked, stacked, lax.Precision.HIGH)
    proj = tmat(stacked, jacobian, lax.Precision.HIGH)
    width = basis.shape[1]
    parts = proj.reshape(3, 128, 8, 128).transpose(0, 2, 1, 3).reshape(3, ROWS, 128)
    cuts = [full[128 * i : 128 * (i + 1), 128 * j : 128 * (j + 1)] for i in range(3) for j in range(i + 1)]
    packed = jnp.concatenate(cuts + [jnp.zeros((ROWS - 768, 128), jnp.float32)], axis=0)
    summed = sum_all(jnp.concatenate([parts, packed[None]], axis=0))
    proj = summed[:3].reshape(3, 8, 128, 128).transpose(0, 2, 1, 3).reshape(384, ROWS)
    cut = {}
    at = 0
    for i in range(3):
        for j in range(i + 1):
            cut[i, j] = summed[3, at : at + 128]
            cut[j, i] = cut[i, j].T
            at += 128
    full = jnp.concatenate([jnp.concatenate([cut[i, j] for j in range(3)], axis=1) for i in range(3)], axis=0)
    hess = mat(proj, proj.T) * scale
    inverse = inverse_lower(combine(full * scale, hess, width))
    return lax.dot_general(
        stacked,
        inverse,
        (((1,), (1,)), ((), ())),
        precision=lax.Precision.HIGH,
        preferred_element_type=jnp.float32,
    )


def solution(mesh):
    placed = (P(("rows", "cols"), None), P(("rows", "cols"), None), P(("rows", "cols"), None))
    return jax.shard_map(
        local, mesh=mesh, in_specs=placed, out_specs=P(("rows", "cols"), None), check_vma=False
    )
```

```python
import functools

import jax
import jax.numpy as jnp
from jax import lax
from jax.experimental import pallas as pl
from jax.experimental.pallas import tpu as pltpu
from jax.sharding import PartitionSpec as P

SIDE = 4
STREAMS = 4
ORDERS = ((0, 1, 2), (1, 2, 0), (2, 0, 1), (0, 2, 1))
OFFSETS = (2, 1, 3)
ROWS = 1024


def sum_kernel(y_ref, out_ref, z0, r0, z1, r1, z2, r2, r3, s0, t0, s1, t1):
    row, col = lax.axis_index("rows"), lax.axis_index("cols")
    core = lax.rem(row, 2)
    place = (lax.div(row, 2 * SIDE), col, lax.rem(lax.div(row, 2), SIDE))

    def device(coords, which):
        return (coords[0] * (2 * SIDE) + coords[2] * 2 + which, coords[1])

    def peer(axis, offset):
        coords = list(place)
        coords[axis] = lax.rem(place[axis] + offset, SIDE)
        return coords

    partner = device(place, 1 - core)
    barrier = pltpu.get_barrier_semaphore()
    pl.semaphore_signal(barrier, inc=1, device_id=partner, device_id_type=pl.DeviceIdType.MESH)
    for axis in range(3):
        for offset in OFFSETS:
            pl.semaphore_signal(
                barrier, inc=1, device_id=device(peer(axis, offset), core), device_id_type=pl.DeviceIdType.MESH
            )
    pl.semaphore_wait(barrier, 1 + 3 * len(OFFSETS))

    sent = []

    def send(src, dst, send_sem, recv_sem, target):
        copy = pltpu.make_async_remote_copy(
            src_ref=src,
            dst_ref=dst,
            send_sem=send_sem,
            recv_sem=recv_sem,
            device_id=target,
            device_id_type=pl.DeviceIdType.MESH,
        )
        copy.start()
        sent.append(copy)
        return copy

    half = ROWS // 2
    order = (3, 0, 1, 2)
    mine = pl.multiple_of(core * half, half)
    other = pl.multiple_of((1 - core) * half, half)
    stage = {}
    for s in order:
        stage[s] = send(y_ref.at[s, pl.ds(other, half)], r0.at[s], s0.at[0, s], t0.at[0, s], partner)

    size = half
    parts = (r1, r2, r3)
    for phase in range(3):
        size //= SIDE
        nxt = {}
        for s in order:
            axis = ORDERS[s][phase]
            if phase == 0:
                stage[s].wait_recv()
                z0[s] = y_ref[s, pl.ds(mine, half)] + r0[s]
            else:
                for copy in stage[s]:
                    copy.wait_recv()
                before = ORDERS[s][phase - 1]
                prev, got = (z0, r1) if phase == 1 else (z1, r2)
                start = pl.multiple_of(place[before] * (size * SIDE), size * SIDE)
                dest = z1 if phase == 1 else z2
                dest[s] = prev[s, pl.ds(start, size * SIDE)] + got[s, 0] + got[s, 1] + got[s, 2]
            src = (z0, z1, z2)[phase]
            nxt[s] = []
            for slot, offset in enumerate(OFFSETS):
                coords = peer(axis, offset)
                start = pl.multiple_of(coords[axis] * size, size)
                nxt[s].append(
                    send(
                        src.at[s, pl.ds(start, size)],
                        parts[phase].at[s, slot],
                        s1.at[phase, s, slot],
                        t1.at[phase, s, slot],
                        device(coords, core),
                    )
                )
        stage = nxt

    for phase in range(3):
        back = 2 - phase
        nxt = {}
        for s in order:
            axis = ORDERS[s][back]
            for copy in stage[s]:
                copy.wait_recv()
            start = mine
            width = half
            for done in range(back + 1):
                width //= SIDE
                start = start + place[ORDERS[s][done]] * width
            start = pl.multiple_of(start, width)
            if phase == 0:
                own = pl.multiple_of(place[axis] * width, width)
                out_ref[s, pl.ds(start, width)] = z2[s, pl.ds(own, width)] + r3[s, 0] + r3[s, 1] + r3[s, 2]
            nxt[s] = []
            for slot, offset in enumerate(OFFSETS):
                nxt[s].append(
                    send(
                        out_ref.at[s, pl.ds(start, width)],
                        out_ref.at[s, pl.ds(start, width)],
                        s1.at[3 + phase, s, slot],
                        t1.at[3 + phase, s, slot],
                        device(peer(axis, offset), core),
                    )
                )
        stage = nxt
    last = []
    for s in order:
        for copy in stage[s]:
            copy.wait_recv()
        last.append(send(out_ref.at[s, pl.ds(mine, half)], out_ref.at[s, pl.ds(mine, half)], s0.at[1, s], t0.at[1, s], partner))
    for copy in last:
        copy.wait_recv()
    for copy in sent:
        copy.wait_send()


def sum_all(y):
    dma = pltpu.SemaphoreType.DMA
    half = ROWS // 2
    f32 = jnp.float32
    return pl.pallas_call(
        sum_kernel,
        out_shape=jax.ShapeDtypeStruct(y.shape, f32),
        in_specs=[pl.BlockSpec(memory_space=pltpu.VMEM)],
        out_specs=pl.BlockSpec(memory_space=pltpu.VMEM),
        scratch_shapes=[
            pltpu.VMEM((STREAMS, half, 128), f32),
            pltpu.VMEM((STREAMS, half, 128), f32),
            pltpu.VMEM((STREAMS, half // 4, 128), f32),
            pltpu.VMEM((STREAMS, 3, half // 4, 128), f32),
            pltpu.VMEM((STREAMS, half // 16, 128), f32),
            pltpu.VMEM((STREAMS, 3, half // 16, 128), f32),
            pltpu.VMEM((STREAMS, 3, half // 64, 128), f32),
            dma((2, STREAMS)),
            dma((2, STREAMS)),
            dma((6, STREAMS, 3)),
            dma((6, STREAMS, 3)),
        ],
        compiler_params=pltpu.CompilerParams(collective_id=0, has_side_effects=True, vmem_limit_bytes=20 * 1024 * 1024),
        name="sum_all",
    )(y)


def mat(left, right, precision=lax.Precision.HIGHEST):
    return jnp.dot(left, right, precision=precision, preferred_element_type=jnp.float32)


def tmat(left, right, precision=lax.Precision.HIGHEST):
    return lax.dot_general(
        left,
        right,
        (((0,), (0,)), ((), ())),
        precision=precision,
        preferred_element_type=jnp.float32,
    )


LEAF = 16
PIECES = 8


def split3(value):
    high = value.astype(jnp.bfloat16)
    rest = value - high.astype(jnp.float32)
    middle = rest.astype(jnp.bfloat16)
    low = (rest - middle.astype(jnp.float32)).astype(jnp.bfloat16)
    return high, middle, low


def split2(value):
    high = value.astype(jnp.bfloat16)
    return high, (value - high.astype(jnp.float32)).astype(jnp.bfloat16)


def nt(left, right):
    return lax.dot_general(left, right, (((1,), (1,)), ((), ())), preferred_element_type=jnp.float32)


def build(y_ref, scale):
    cut = {}
    at = 0
    for i in range(3):
        for j in range(i + 1):
            cut[i, j] = y_ref[3, at : at + 128] * scale
            at += 128
    s_vv = jnp.concatenate(
        [jnp.concatenate([cut[0, 0], cut[1, 0].T], axis=1), jnp.concatenate([cut[1, 0], cut[1, 1]], axis=1)], axis=0
    )
    s_vw = jnp.concatenate([cut[2, 0].T, cut[2, 1].T], axis=0)
    summed = s_vw + (s_vw - mat(s_vv, s_vw))
    cross = tmat(summed, s_vw)
    last = cut[2, 2] - cross - cross.T + tmat(summed, mat(s_vv, summed) + summed)
    hess = jnp.zeros((384, 384), jnp.float32)
    for pair in range(0, 8, 2):
        rows = [
            jnp.concatenate([y_ref[s, 128 * t : 128 * (t + 1)] for s in range(3)], axis=0) for t in (pair, pair + 1)
        ]
        high, low = split2(jnp.concatenate(rows, axis=1))
        hess = hess + (nt(high, low) + nt(low, high) + nt(high, high))
    hess = hess * scale
    ident = jnp.where(
        lax.broadcasted_iota(jnp.int32, (256, 256), 0) == lax.broadcasted_iota(jnp.int32, (256, 256), 1), 1.0, 0.0
    ).astype(jnp.float32)
    top = jnp.concatenate([ident, summed], axis=1)
    low = jnp.concatenate([summed.T, last], axis=1)
    return jnp.concatenate([top, low], axis=0) + hess


def leaf_step(a, block, step):
    tiles = LEAF // 8
    width = a.shape[1]
    first = pl.multiple_of(block * 128 + step * LEAF, LEAF)
    base = pl.multiple_of(block * 128, 128)
    sub = lax.broadcasted_iota(jnp.int32, (8, 128), 0)
    lane = lax.broadcasted_iota(jnp.int32, (8, 128), 1)
    columns = {}
    for t in range(tiles):
        diag = a[pl.ds(first + 8 * t, 8), pl.ds(base, 128)]
        for k in range(min(LEAF, 8 * (t + 1))):
            at = step * LEAF + k
            columns[k, t] = jnp.broadcast_to(diag[:, at : at + 1], (8, 128))
    panel = {}
    for t in range(tiles):
        for c in range(width // 128):
            place = lane + (128 * c - first)
            own = (place >= 0) & (place < LEAF)
            unit = jnp.where(place == sub + 8 * t, 1.0, 0.0)
            panel[t, c] = jnp.where(own, unit, a[pl.ds(first + 8 * t, 8), 128 * c : 128 * (c + 1)])
    factor = [jnp.zeros((8, 128), jnp.float32) for _ in range(tiles)]
    for j in range(LEAF):
        home, row = j // 8, j % 8
        pivot = jnp.broadcast_to(columns[j, home][row : row + 1], (8, 128))
        root = lax.rsqrt(pivot)
        inverse = root * root
        factor[home] = jnp.where(sub == row, root, factor[home])
        if j + 1 == LEAF:
            break
        mult = {}
        for t in range(home, tiles):
            value = columns[j, t] * inverse
            if t == home:
                value = jnp.where(sub > row, value, 0.0)
            mult[t] = value
        for k in range(j + 1, LEAF):
            spread = jnp.broadcast_to(columns[j, k // 8][k % 8 : k % 8 + 1], (8, 128))
            for t in range(k // 8, tiles):
                if k == j + 1:
                    columns[k, t] = columns[k, t] - (columns[j, t] * spread) * inverse
                else:
                    columns[k, t] = columns[k, t] - mult[t] * spread
        for c in range(width // 128):
            spread = jnp.broadcast_to(panel[home, c][row : row + 1], (8, 128))
            for t in range(home, tiles):
                panel[t, c] = panel[t, c] - mult[t] * spread
    rows = jnp.concatenate(
        [
            jnp.concatenate([panel[t, c] * factor[t] for c in range(width // 128)], axis=1)
            for t in range(tiles)
        ],
        axis=0,
    )
    place = lax.broadcasted_iota(jnp.int32, (LEAF, width), 1) - first
    right = split3(rows)
    left = split3(jnp.where(place >= LEAF, rows, 0.0))
    none = jnp.zeros((LEAF, width), jnp.bfloat16)
    pick = lambda parts, order: jnp.concatenate([parts[i] for i in order] + [none] * (PIECES - len(order)), axis=0)
    update = lax.dot_general(
        pick(left, (0, 0, 1, 0, 2, 1)),
        pick(right, (0, 1, 0, 2, 0, 1)),
        (((0,), (0,)), ((), ())),
        preferred_element_type=jnp.float32,
    )
    place = lax.broadcasted_iota(jnp.int32, (width, width), 1) - first
    own = (place >= 0) & (place < LEAF)
    a[...] = jnp.where(own, 0.0, a[...]) - update
    a[pl.ds(first, LEAF), :] = rows


def factor_kernel(scale, y_ref, a):
    a[...] = build(y_ref, scale)

    def block_step(block, _):
        for step in range(128 // LEAF):
            leaf_step(a, block, step)
        return 0

    lax.fori_loop(0, a.shape[0] // 128, block_step, 0)


def factor_inverse(summed, scale):
    return pl.pallas_call(
        functools.partial(factor_kernel, scale),
        out_shape=jax.ShapeDtypeStruct((384, 384), jnp.float32),
        in_specs=[pl.BlockSpec(memory_space=pltpu.VMEM)],
        out_specs=pl.BlockSpec(memory_space=pltpu.VMEM),
        compiler_params=pltpu.CompilerParams(vmem_limit_bytes=32 * 1024 * 1024),
        name="factor_inverse",
    )(summed)


def local(basis, new_vectors, jacobian):
    total = basis.shape[0] * lax.axis_size("rows") * lax.axis_size("cols")
    scale = 1.0 / total
    width = basis.shape[1]
    stacked = jnp.concatenate([basis, new_vectors], axis=1)
    full = tmat(stacked, stacked, lax.Precision.HIGH)
    proj = tmat(stacked, jacobian, lax.Precision.HIGH)
    width = basis.shape[1]
    parts = proj.reshape(3, 128, 8, 128).transpose(0, 2, 1, 3).reshape(3, ROWS, 128)
    cuts = [full[128 * i : 128 * (i + 1), 128 * j : 128 * (j + 1)] for i in range(3) for j in range(i + 1)]
    packed = jnp.concatenate(cuts + [jnp.zeros((ROWS - 768, 128), jnp.float32)], axis=0)
    summed = sum_all(jnp.concatenate([parts, packed[None]], axis=0))
    inverse = factor_inverse(summed, scale)
    return lax.dot_general(
        stacked,
        inverse,
        (((1,), (1,)), ((), ())),
        precision=lax.Precision.HIGH,
        preferred_element_type=jnp.float32,
    )


def solution(mesh):
    placed = (P(("rows", "cols"), None), P(("rows", "cols"), None), P(("rows", "cols"), None))
    return jax.shard_map(
        local, mesh=mesh, in_specs=placed, out_specs=P(("rows", "cols"), None), check_vma=False
    )
```

```python
import functools

import jax
import jax.numpy as jnp
from jax import lax
from jax.experimental import pallas as pl
from jax.experimental.pallas import tpu as pltpu
from jax.sharding import PartitionSpec as P

SIDE = 4
STREAMS = 4
AXIS = (0, 1, 2, 0)
OFFSETS = (2, 1, 3, 0)
PLANE = sorted(
    [(b, c) for b in range(SIDE) for c in range(SIDE) if b or c],
    key=lambda at: -(min(at[0], SIDE - at[0]) + min(at[1], SIDE - at[1])),
)
ROWS = 1024
HALF = ROWS // 2
PART = HALF // SIDE
PIECE = PART // SIDE**2
ORDER = (3, 0, 1, 2)


class Links:
    def __init__(self):
        row, col = lax.axis_index("rows"), lax.axis_index("cols")
        self.core = lax.rem(row, 2)
        self.place = (lax.div(row, 2 * SIDE), col, lax.rem(lax.div(row, 2), SIDE))
        self.partner = self.device(self.place, 1 - self.core)
        self.sent = []

    def device(self, coords, which):
        return (coords[0] * (2 * SIDE) + coords[2] * 2 + which, coords[1])

    def moved(self, axes, offsets):
        coords = list(self.place)
        for axis, offset in zip(axes, offsets):
            coords[axis] = lax.rem(self.place[axis] + offset, SIDE)
        return coords

    def greet(self):
        barrier = pltpu.get_barrier_semaphore()
        others = [self.partner]
        for axis in range(3):
            others += [self.device(self.moved((axis,), (offset,)), self.core) for offset in OFFSETS[:3]]
        for axes in ((1, 2), (0, 2), (0, 1)):
            others += [self.device(self.moved(axes, at), self.core) for at in PLANE if at[0] and at[1]]
        for other in others:
            pl.semaphore_signal(barrier, inc=1, device_id=other, device_id_type=pl.DeviceIdType.MESH)
        self.greeted = (barrier, len(others))

    def meet(self):
        pl.semaphore_wait(*self.greeted)

    def send(self, src, dst, sems, at, target):
        copy = pltpu.make_async_remote_copy(
            src_ref=src,
            dst_ref=dst,
            send_sem=sems[0].at[at],
            recv_sem=sems[1].at[at],
            device_id=target,
            device_id_type=pl.DeviceIdType.MESH,
        )
        copy.start()
        self.sent.append(copy)
        return copy


def plane_of(s):
    return tuple(axis for axis in range(3) if axis != AXIS[s])


def share_core(links, s, y_ref, r0, sems):
    copies = []
    for slot, offset in enumerate(OFFSETS):
        at = links.moved((AXIS[s],), (offset,))[AXIS[s]] * PART
        rows = pl.ds(pl.multiple_of((1 - links.core) * HALF + at, PART), PART)
        keep = pl.ds(pl.multiple_of(at, PART), PART)
        copies.append(links.send(y_ref.at[s, rows], r0.at[s, keep], sems, (s, slot), links.partner))
    return copies


def share_line(links, s, waits, y_ref, r0, z0, r1, sems):
    copies = []
    for slot, offset in enumerate(OFFSETS):
        coords = links.moved((AXIS[s],), (offset,))
        at = coords[AXIS[s]] * PART
        rows = pl.ds(pl.multiple_of(links.core * HALF + at, PART), PART)
        keep = pl.ds(pl.multiple_of(at, PART), PART)
        waits[slot].wait_recv()
        z0[s, slot] = y_ref[s, rows] + r0[s, keep]
        if offset:
            copies.append(links.send(z0.at[s, slot], r1.at[s, slot], sems, (s, slot), links.device(coords, links.core)))
    return copies


def share_plane(links, s, waits, z0, r1, z1, r2, sems):
    for copy in waits:
        copy.wait_recv()
    z1[s] = (z0[s, 3] + r1[s, 0]) + (r1[s, 1] + r1[s, 2])
    copies = []
    axes = plane_of(s)
    for slot, offsets in enumerate(PLANE):
        coords = links.moved(axes, offsets)
        at = pl.multiple_of((coords[axes[0]] * SIDE + coords[axes[1]]) * PIECE, PIECE)
        copies.append(
            links.send(z1.at[s, pl.ds(at, PIECE)], r2.at[s, slot], sems, (s, slot), links.device(coords, links.core))
        )
    return copies


def spread_plane(links, s, waits, z1, r2, out_ref, sems):
    for copy in waits:
        copy.wait_recv()
    axes = plane_of(s)
    at = (links.place[axes[0]] * SIDE + links.place[axes[1]]) * PIECE
    parts = [z1[s, pl.ds(pl.multiple_of(at, PIECE), PIECE)]] + [r2[s, slot] for slot in range(len(PLANE))]
    while len(parts) > 1:
        parts = [left + right for left, right in zip(parts[::2], parts[1::2])]
    rows = pl.ds(pl.multiple_of(links.core * HALF + links.place[AXIS[s]] * PART + at, PIECE), PIECE)
    out_ref[s, rows] = parts[0]
    return [
        links.send(
            out_ref.at[s, rows],
            out_ref.at[s, rows],
            sems,
            (s, slot),
            links.device(links.moved(axes, offsets), links.core),
        )
        for slot, offsets in enumerate(PLANE)
    ]


def spread_line(links, s, waits, out_ref, sems, core_sems):
    for copy in waits:
        copy.wait_recv()
    rows = pl.ds(pl.multiple_of(links.core * HALF + links.place[AXIS[s]] * PART, PART), PART)
    block = out_ref.at[s, rows]
    copies = [
        links.send(block, block, sems, (s, slot), links.device(links.moved((AXIS[s],), (offset,)), links.core))
        for slot, offset in enumerate(OFFSETS[:3])
    ]
    return copies, [links.send(block, block, core_sems, (s, 3), links.partner)]


def spread_core(links, s, waits, out_ref, core_sems):
    copies = []
    for slot in (1, 2, 0):
        waits[slot].wait_recv()
        at = links.moved((AXIS[s],), (SIDE - OFFSETS[slot],))[AXIS[s]] * PART
        block = out_ref.at[s, pl.ds(pl.multiple_of(links.core * HALF + at, PART), PART)]
        copies.append(links.send(block, block, core_sems, (s, slot), links.partner))
    return copies


def split3(value):
    high = value.astype(jnp.bfloat16)
    rest = value - high.astype(jnp.float32)
    middle = rest.astype(jnp.bfloat16)
    low = (rest - middle.astype(jnp.float32)).astype(jnp.bfloat16)
    return high, middle, low


def split2(value):
    high = value.astype(jnp.bfloat16)
    return high, (value - high.astype(jnp.float32)).astype(jnp.bfloat16)


CHUNK = 512


def mm(left, right):
    return jnp.dot(left, right, preferred_element_type=jnp.float32)


def gram_and_project(v_ref, w_ref, j_ref, out_ref, s_buf, j_buf, high_t, low_t, g_acc, y_ref, z0, r0, r1, z1, r2, in_s, in_j, *sems):
    sems = [sems[i : i + 2] for i in range(0, 12, 2)]
    links = Links()
    links.greet()
    width, block = v_ref.shape[1], w_ref.shape[1]
    joint = width + block
    chunks = v_ref.shape[0] // CHUNK
    sides = [pl.multiple_of(which * HALF, HALF) for which in (1 - links.core, links.core)]

    def load_s(k):
        rows = pl.ds(pl.multiple_of(k * CHUNK, CHUNK), CHUNK)
        return (
            pltpu.make_async_copy(v_ref.at[rows], s_buf.at[rows, pl.ds(0, width)], in_s.at[0, k]),
            pltpu.make_async_copy(w_ref.at[rows], s_buf.at[rows, pl.ds(width, block)], in_s.at[1, k]),
        )

    def load_j(side, k):
        rows = pl.ds(pl.multiple_of(k * CHUNK, CHUNK), CHUNK)
        return pltpu.make_async_copy(j_ref.at[rows, pl.ds(sides[side], HALF)], j_buf.at[side, rows], in_j.at[side, k])

    for k in range(chunks):
        for copy in load_s(k):
            copy.start()
    for side in range(2):
        for k in range(chunks):
            load_j(side, k).start()
    g_acc[...] = jnp.zeros_like(g_acc)
    y_ref[...] = jnp.zeros_like(y_ref)

    def gram_step(k, _):
        for copy in load_s(k):
            copy.wait()
        rows = pl.ds(pl.multiple_of(k * CHUNK, CHUNK), CHUNK)
        value = s_buf[rows]
        flipped = split2(value.T)
        high_t[:, rows], low_t[:, rows] = flipped
        g_acc[...] += mm(flipped[0], jnp.concatenate(split2(value), axis=1))
        return 0

    lax.fori_loop(0, chunks, gram_step, 0)
    at = 0
    for i in range(3):
        for j in range(i + 1):
            tile = g_acc[128 * i : 128 * (i + 1), 128 * j : 128 * (j + 1)]
            mixed = g_acc[128 * i : 128 * (i + 1), joint + 128 * j : joint + 128 * (j + 1)]
            other = g_acc[128 * j : 128 * (j + 1), joint + 128 * i : joint + 128 * (i + 1)]
            y_ref[3, at : at + 128] = tile + (mixed + other.T)
            at += 128

    def project(side):
        def step(k, _):
            load_j(side, k).wait()
            rows = pl.ds(pl.multiple_of(k * CHUNK, CHUNK), CHUNK)
            high, low = split2(j_buf[side, rows])
            lead = high_t[:, rows]
            value = mm(lead, low) + mm(low_t[:, rows], high) + mm(lead, high)
            for s in range(3):
                for t in range(SIDE):
                    at = pl.ds(pl.multiple_of(sides[side] + 128 * t, 128), 128)
                    y_ref[s, at] += value[128 * s : 128 * (s + 1), 128 * t : 128 * (t + 1)]
            return 0

        lax.fori_loop(0, chunks, step, 0)

    links.meet()
    stage = {3: share_core(links, 3, y_ref, r0, sems[0])}
    project(0)
    for s in range(3):
        stage[s] = share_core(links, s, y_ref, r0, sems[0])
    stage[3] = share_line(links, 3, stage[3], y_ref, r0, z0, r1, sems[1])
    project(1)
    stage[3] = share_plane(links, 3, stage[3], z0, r1, z1, r2, sems[2])
    for s in range(3):
        stage[s] = share_line(links, s, stage[s], y_ref, r0, z0, r1, sems[1])
    stage[3] = spread_plane(links, 3, stage[3], z1, r2, out_ref, sems[3])
    for s in range(3):
        stage[s] = share_plane(links, s, stage[s], z0, r1, z1, r2, sems[2])
    last = []
    stage[3], own = spread_line(links, 3, stage[3], out_ref, sems[4], sems[5])
    last += own
    for s in range(3):
        stage[s] = spread_plane(links, s, stage[s], z1, r2, out_ref, sems[3])
    last += spread_core(links, 3, stage[3], out_ref, sems[5])
    for s in range(3):
        stage[s], own = spread_line(links, s, stage[s], out_ref, sems[4], sems[5])
        last += own
    for s in range(3):
        last += spread_core(links, s, stage[s], out_ref, sems[5])
    for copy in last:
        copy.wait_recv()
    for copy in links.sent:
        copy.wait_send()


def summed_products(basis, new_vectors, jacobian):
    f32, bf16, dma = jnp.float32, jnp.bfloat16, pltpu.SemaphoreType.DMA
    rows = basis.shape[0]
    joint = basis.shape[1] + new_vectors.shape[1]
    sems = []
    for count in (4, 3, len(PLANE), len(PLANE), 3, 4):
        sems += [dma((STREAMS, count))] * 2
    return pl.pallas_call(
        gram_and_project,
        out_shape=jax.ShapeDtypeStruct((STREAMS, ROWS, 128), f32),
        in_specs=[pl.BlockSpec(memory_space=pltpu.HBM)] * 3,
        out_specs=pl.BlockSpec(memory_space=pltpu.VMEM),
        scratch_shapes=[
            pltpu.VMEM((rows, joint), f32),
            pltpu.VMEM((2, rows, HALF), f32),
            pltpu.VMEM((joint, rows), bf16),
            pltpu.VMEM((joint, rows), bf16),
            pltpu.VMEM((joint, 2 * joint), f32),
            pltpu.VMEM((STREAMS, ROWS, 128), f32),
            pltpu.VMEM((STREAMS, SIDE, PART, 128), f32),
            pltpu.VMEM((STREAMS, HALF, 128), f32),
            pltpu.VMEM((STREAMS, 3, PART, 128), f32),
            pltpu.VMEM((STREAMS, PART, 128), f32),
            pltpu.VMEM((STREAMS, len(PLANE), PIECE, 128), f32),
            dma((2, rows // CHUNK)),
            dma((2, rows // CHUNK)),
        ]
        + sems,
        compiler_params=pltpu.CompilerParams(
            collective_id=0, has_side_effects=True, vmem_limit_bytes=48 * 1024 * 1024
        ),
        name="summed_products",
    )(basis, new_vectors, jacobian)


def mat(left, right, precision=lax.Precision.HIGHEST):
    return jnp.dot(left, right, precision=precision, preferred_element_type=jnp.float32)


def tmat(left, right, precision=lax.Precision.HIGHEST):
    return lax.dot_general(
        left,
        right,
        (((0,), (0,)), ((), ())),
        precision=precision,
        preferred_element_type=jnp.float32,
    )


LEAF = 16
PIECES = 8


def nt(left, right):
    return lax.dot_general(left, right, (((1,), (1,)), ((), ())), preferred_element_type=jnp.float32)


def build(y_ref, scale):
    cut = {}
    at = 0
    for i in range(3):
        for j in range(i + 1):
            cut[i, j] = y_ref[3, at : at + 128] * scale
            at += 128
    s_vv = jnp.concatenate(
        [jnp.concatenate([cut[0, 0], cut[1, 0].T], axis=1), jnp.concatenate([cut[1, 0], cut[1, 1]], axis=1)], axis=0
    )
    s_vw = jnp.concatenate([cut[2, 0].T, cut[2, 1].T], axis=0)
    summed = s_vw + (s_vw - mat(s_vv, s_vw))
    cross = tmat(summed, s_vw)
    last = cut[2, 2] - cross - cross.T + tmat(summed, mat(s_vv, summed) + summed)
    hess = jnp.zeros((384, 384), jnp.float32)
    for pair in range(0, 8, 2):
        rows = [
            jnp.concatenate([y_ref[s, 128 * t : 128 * (t + 1)] for s in range(3)], axis=0) for t in (pair, pair + 1)
        ]
        high, low = split2(jnp.concatenate(rows, axis=1))
        hess = hess + (nt(high, low) + nt(low, high) + nt(high, high))
    hess = hess * scale
    ident = jnp.where(
        lax.broadcasted_iota(jnp.int32, (256, 256), 0) == lax.broadcasted_iota(jnp.int32, (256, 256), 1), 1.0, 0.0
    ).astype(jnp.float32)
    top = jnp.concatenate([ident, summed], axis=1)
    low = jnp.concatenate([summed.T, last], axis=1)
    return jnp.concatenate([top, low], axis=0) + hess


def leaf_step(a, block, step):
    tiles = LEAF // 8
    width = a.shape[1]
    first = pl.multiple_of(block * 128 + step * LEAF, LEAF)
    base = pl.multiple_of(block * 128, 128)
    sub = lax.broadcasted_iota(jnp.int32, (8, 128), 0)
    lane = lax.broadcasted_iota(jnp.int32, (8, 128), 1)
    columns = {}
    for t in range(tiles):
        diag = a[pl.ds(first + 8 * t, 8), pl.ds(base, 128)]
        for k in range(min(LEAF, 8 * (t + 1))):
            at = step * LEAF + k
            columns[k, t] = jnp.broadcast_to(diag[:, at : at + 1], (8, 128))
    panel = {}
    for t in range(tiles):
        for c in range(width // 128):
            place = lane + (128 * c - first)
            own = (place >= 0) & (place < LEAF)
            unit = jnp.where(place == sub + 8 * t, 1.0, 0.0)
            panel[t, c] = jnp.where(own, unit, a[pl.ds(first + 8 * t, 8), 128 * c : 128 * (c + 1)])
    factor = [jnp.zeros((8, 128), jnp.float32) for _ in range(tiles)]
    for j in range(LEAF):
        home, row = j // 8, j % 8
        pivot = jnp.broadcast_to(columns[j, home][row : row + 1], (8, 128))
        root = lax.rsqrt(pivot)
        inverse = root * root
        factor[home] = jnp.where(sub == row, root, factor[home])
        if j + 1 == LEAF:
            break
        mult = {}
        for t in range(home, tiles):
            value = columns[j, t] * inverse
            if t == home:
                value = jnp.where(sub > row, value, 0.0)
            mult[t] = value
        for k in range(j + 1, LEAF):
            spread = jnp.broadcast_to(columns[j, k // 8][k % 8 : k % 8 + 1], (8, 128))
            for t in range(k // 8, tiles):
                if k == j + 1:
                    columns[k, t] = columns[k, t] - (columns[j, t] * spread) * inverse
                else:
                    columns[k, t] = columns[k, t] - mult[t] * spread
        for c in range(width // 128):
            spread = jnp.broadcast_to(panel[home, c][row : row + 1], (8, 128))
            for t in range(home, tiles):
                panel[t, c] = panel[t, c] - mult[t] * spread
    rows = jnp.concatenate(
        [
            jnp.concatenate([panel[t, c] * factor[t] for c in range(width // 128)], axis=1)
            for t in range(tiles)
        ],
        axis=0,
    )
    place = lax.broadcasted_iota(jnp.int32, (LEAF, width), 1) - first
    right = split3(rows)
    left = split3(jnp.where(place >= LEAF, rows, 0.0))
    none = jnp.zeros((LEAF, width), jnp.bfloat16)
    pick = lambda parts, order: jnp.concatenate([parts[i] for i in order] + [none] * (PIECES - len(order)), axis=0)
    update = lax.dot_general(
        pick(left, (0, 0, 1, 0, 2, 1)),
        pick(right, (0, 1, 0, 2, 0, 1)),
        (((0,), (0,)), ((), ())),
        preferred_element_type=jnp.float32,
    )
    place = lax.broadcasted_iota(jnp.int32, (width, width), 1) - first
    own = (place >= 0) & (place < LEAF)
    a[...] = jnp.where(own, 0.0, a[...]) - update
    a[pl.ds(first, LEAF), :] = rows


def factor_kernel(scale, y_ref, a):
    a[...] = build(y_ref, scale)

    def block_step(block, _):
        for step in range(128 // LEAF):
            leaf_step(a, block, step)
        return 0

    lax.fori_loop(0, a.shape[0] // 128, block_step, 0)


def factor_inverse(summed, scale):
    return pl.pallas_call(
        functools.partial(factor_kernel, scale),
        out_shape=jax.ShapeDtypeStruct((384, 384), jnp.float32),
        in_specs=[pl.BlockSpec(memory_space=pltpu.VMEM)],
        out_specs=pl.BlockSpec(memory_space=pltpu.VMEM),
        compiler_params=pltpu.CompilerParams(vmem_limit_bytes=32 * 1024 * 1024),
        name="factor_inverse",
    )(summed)


def local(basis, new_vectors, jacobian):
    total = basis.shape[0] * lax.axis_size("rows") * lax.axis_size("cols")
    scale = 1.0 / total
    stacked = jnp.concatenate([basis, new_vectors], axis=1)
    summed = summed_products(basis, new_vectors, jacobian)
    inverse = factor_inverse(summed, scale)
    return lax.dot_general(
        stacked,
        inverse,
        (((1,), (1,)), ((), ())),
        precision=lax.Precision.HIGH,
        preferred_element_type=jnp.float32,
    )


def solution(mesh):
    placed = (P(("rows", "cols"), None), P(("rows", "cols"), None), P(("rows", "cols"), None))
    return jax.shard_map(
        local, mesh=mesh, in_specs=placed, out_specs=P(("rows", "cols"), None), check_vma=False
    )
```

```python
import functools

import jax
import jax.numpy as jnp
from jax import lax
from jax.experimental import pallas as pl
from jax.experimental.pallas import tpu as pltpu
from jax.sharding import PartitionSpec as P

SIDE = 4
STREAMS = 4
AXIS = (0, 1, 2, 0)
OFFSETS = (2, 1, 3, 0)
PLANE = sorted(
    [(b, c) for b in range(SIDE) for c in range(SIDE) if b or c],
    key=lambda at: -(min(at[0], SIDE - at[0]) + min(at[1], SIDE - at[1])),
)
ROWS = 1024
VMEM_LIMIT = 55_000_000
HALF = ROWS // 2
PART = HALF // SIDE
PIECE = PART // SIDE**2
ORDER = (3, 0, 1, 2)


class Links:
    def __init__(self):
        row, col = lax.axis_index("rows"), lax.axis_index("cols")
        self.core = lax.rem(row, 2)
        self.place = (lax.div(row, 2 * SIDE), col, lax.rem(lax.div(row, 2), SIDE))
        self.partner = self.device(self.place, 1 - self.core)
        self.sent = []

    def device(self, coords, which):
        return (coords[0] * (2 * SIDE) + coords[2] * 2 + which, coords[1])

    def moved(self, axes, offsets):
        coords = list(self.place)
        for axis, offset in zip(axes, offsets):
            coords[axis] = lax.rem(self.place[axis] + offset, SIDE)
        return coords

    def greet(self):
        barrier = pltpu.get_barrier_semaphore()
        others = [self.partner]
        for axis in range(3):
            others += [self.device(self.moved((axis,), (offset,)), self.core) for offset in OFFSETS[:3]]
        for axes in ((1, 2), (0, 2), (0, 1)):
            others += [self.device(self.moved(axes, at), self.core) for at in PLANE if at[0] and at[1]]
        for other in others:
            pl.semaphore_signal(barrier, inc=1, device_id=other, device_id_type=pl.DeviceIdType.MESH)
        self.greeted = (barrier, len(others))

    def meet(self):
        pl.semaphore_wait(*self.greeted)

    def send(self, src, dst, sems, at, target):
        copy = pltpu.make_async_remote_copy(
            src_ref=src,
            dst_ref=dst,
            send_sem=sems[0].at[at],
            recv_sem=sems[1].at[at],
            device_id=target,
            device_id_type=pl.DeviceIdType.MESH,
        )
        copy.start()
        self.sent.append(copy)
        return copy


def plane_of(s):
    return tuple(axis for axis in range(3) if axis != AXIS[s])


def share_core(links, s, y_ref, r0, sems):
    copies = []
    for slot, offset in enumerate(OFFSETS):
        at = links.moved((AXIS[s],), (offset,))[AXIS[s]] * PART
        rows = pl.ds(pl.multiple_of((1 - links.core) * HALF + at, PART), PART)
        keep = pl.ds(pl.multiple_of(at, PART), PART)
        copies.append(links.send(y_ref.at[s, rows], r0.at[s, keep], sems, (s, slot), links.partner))
    return copies


def share_line(links, s, waits, y_ref, r0, z0, r1, sems):
    copies = []
    for slot, offset in enumerate(OFFSETS):
        coords = links.moved((AXIS[s],), (offset,))
        at = coords[AXIS[s]] * PART
        rows = pl.ds(pl.multiple_of(links.core * HALF + at, PART), PART)
        keep = pl.ds(pl.multiple_of(at, PART), PART)
        waits[slot].wait_recv()
        z0[s, slot] = y_ref[s, rows] + r0[s, keep]
        if offset:
            copies.append(links.send(z0.at[s, slot], r1.at[s, slot], sems, (s, slot), links.device(coords, links.core)))
    return copies


def share_plane(links, s, waits, z0, r1, z1, r2, sems):
    for copy in waits:
        copy.wait_recv()
    z1[s] = (z0[s, 3] + r1[s, 0]) + (r1[s, 1] + r1[s, 2])
    copies = []
    axes = plane_of(s)
    for slot, offsets in enumerate(PLANE):
        coords = links.moved(axes, offsets)
        at = pl.multiple_of((coords[axes[0]] * SIDE + coords[axes[1]]) * PIECE, PIECE)
        copies.append(
            links.send(z1.at[s, pl.ds(at, PIECE)], r2.at[s, slot], sems, (s, slot), links.device(coords, links.core))
        )
    return copies


def spread_plane(links, s, waits, z1, r2, out_ref, sems):
    for copy in waits:
        copy.wait_recv()
    axes = plane_of(s)
    at = (links.place[axes[0]] * SIDE + links.place[axes[1]]) * PIECE
    parts = [z1[s, pl.ds(pl.multiple_of(at, PIECE), PIECE)]] + [r2[s, slot] for slot in range(len(PLANE))]
    while len(parts) > 1:
        parts = [left + right for left, right in zip(parts[::2], parts[1::2])]
    rows = pl.ds(pl.multiple_of(links.core * HALF + links.place[AXIS[s]] * PART + at, PIECE), PIECE)
    out_ref[s, rows] = parts[0]
    return [
        links.send(
            out_ref.at[s, rows],
            out_ref.at[s, rows],
            sems,
            (s, slot),
            links.device(links.moved(axes, offsets), links.core),
        )
        for slot, offsets in enumerate(PLANE)
    ]


def spread_line(links, s, waits, out_ref, sems, core_sems):
    for copy in waits:
        copy.wait_recv()
    rows = pl.ds(pl.multiple_of(links.core * HALF + links.place[AXIS[s]] * PART, PART), PART)
    block = out_ref.at[s, rows]
    copies = [
        links.send(block, block, sems, (s, slot), links.device(links.moved((AXIS[s],), (offset,)), links.core))
        for slot, offset in enumerate(OFFSETS[:3])
    ]
    return copies, [links.send(block, block, core_sems, (s, 3), links.partner)]


def spread_core(links, s, waits, out_ref, core_sems):
    copies = []
    for slot in (1, 2, 0):
        waits[slot].wait_recv()
        at = links.moved((AXIS[s],), (SIDE - OFFSETS[slot],))[AXIS[s]] * PART
        block = out_ref.at[s, pl.ds(pl.multiple_of(links.core * HALF + at, PART), PART)]
        copies.append(links.send(block, block, core_sems, (s, slot), links.partner))
    return copies


def split3(value):
    high = value.astype(jnp.bfloat16)
    rest = value - high.astype(jnp.float32)
    middle = rest.astype(jnp.bfloat16)
    low = (rest - middle.astype(jnp.float32)).astype(jnp.bfloat16)
    return high, middle, low


def split2(value):
    high = value.astype(jnp.bfloat16)
    return high, (value - high.astype(jnp.float32)).astype(jnp.bfloat16)


def mat(left, right, precision=lax.Precision.HIGHEST):
    return jnp.dot(left, right, precision=precision, preferred_element_type=jnp.float32)


def tmat(left, right, precision=lax.Precision.HIGHEST):
    return lax.dot_general(
        left,
        right,
        (((0,), (0,)), ((), ())),
        precision=precision,
        preferred_element_type=jnp.float32,
    )


def gram_part(y_ref, scale):
    cut = {}
    at = 0
    for i in range(3):
        for j in range(i + 1):
            cut[i, j] = y_ref[3, at : at + 128] * scale
            at += 128
    s_vv = jnp.concatenate(
        [jnp.concatenate([cut[0, 0], cut[1, 0].T], axis=1), jnp.concatenate([cut[1, 0], cut[1, 1]], axis=1)], axis=0
    )
    s_vw = jnp.concatenate([cut[2, 0].T, cut[2, 1].T], axis=0)
    summed = s_vw + (s_vw - mat(s_vv, s_vw))
    cross = tmat(summed, s_vw)
    last = cut[2, 2] - cross - cross.T + tmat(summed, mat(s_vv, summed) + summed)
    ident = jnp.where(
        lax.broadcasted_iota(jnp.int32, (256, 256), 0) == lax.broadcasted_iota(jnp.int32, (256, 256), 1), 1.0, 0.0
    ).astype(jnp.float32)
    top = jnp.concatenate([ident, summed], axis=1)
    low = jnp.concatenate([summed.T, last], axis=1)
    return jnp.concatenate([top, low], axis=0)


def nt(left, right):
    return lax.dot_general(left, right, (((1,), (1,)), ((), ())), preferred_element_type=jnp.float32)


def half_square(y_ref, start):
    total = None
    for pair in range(0, HALF, 256):
        blocks = []
        for t in (pair, pair + 128):
            rows = pl.ds(pl.multiple_of(start + t, 128), 128)
            blocks.append(jnp.concatenate([y_ref[s, rows] for s in range(3)], axis=0))
        high, low = split2(jnp.concatenate(blocks, axis=1))
        value = nt(high, low) + nt(low, high) + nt(high, high)
        total = value if total is None else total + value
    return total


CHUNK = 512


def mm(left, right):
    return jnp.dot(left, right, preferred_element_type=jnp.float32)


def gram_and_project(scale, v_ref, w_ref, j_ref, b_ref, out_ref, s_buf, j_buf, high_t, low_t, g_acc, y_ref, z0, r0, r1, z1, r2, in_s, in_j, *sems):
    sems = [sems[i : i + 2] for i in range(0, 12, 2)]
    links = Links()
    links.greet()
    width, block = v_ref.shape[1], w_ref.shape[1]
    joint = width + block
    chunks = v_ref.shape[0] // CHUNK
    sides = [pl.multiple_of(which * HALF, HALF) for which in (1 - links.core, links.core)]

    def load_s(k):
        rows = pl.ds(pl.multiple_of(k * CHUNK, CHUNK), CHUNK)
        return (
            pltpu.make_async_copy(v_ref.at[rows], s_buf.at[rows, pl.ds(0, width)], in_s.at[0, k]),
            pltpu.make_async_copy(w_ref.at[rows], s_buf.at[rows, pl.ds(width, block)], in_s.at[1, k]),
        )

    def load_j(side, k):
        rows = pl.ds(pl.multiple_of(k * CHUNK, CHUNK), CHUNK)
        return pltpu.make_async_copy(j_ref.at[rows, pl.ds(sides[side], HALF)], j_buf.at[side, rows], in_j.at[side, k])

    for k in range(chunks):
        for copy in load_s(k):
            copy.start()
    for side in range(2):
        for k in range(chunks):
            load_j(side, k).start()
    g_acc[...] = jnp.zeros_like(g_acc)
    y_ref[...] = jnp.zeros_like(y_ref)

    def gram_step(k, _):
        for copy in load_s(k):
            copy.wait()
        rows = pl.ds(pl.multiple_of(k * CHUNK, CHUNK), CHUNK)
        value = s_buf[rows]
        flipped = split2(value.T)
        high_t[:, rows], low_t[:, rows] = flipped
        g_acc[...] += mm(flipped[0], jnp.concatenate(split2(value), axis=1))
        return 0

    lax.fori_loop(0, chunks, gram_step, 0)
    at = 0
    for i in range(3):
        for j in range(i + 1):
            tile = g_acc[128 * i : 128 * (i + 1), 128 * j : 128 * (j + 1)]
            mixed = g_acc[128 * i : 128 * (i + 1), joint + 128 * j : joint + 128 * (j + 1)]
            other = g_acc[128 * j : 128 * (j + 1), joint + 128 * i : joint + 128 * (i + 1)]
            y_ref[3, at : at + 128] = tile + (mixed + other.T)
            at += 128

    def project(side):
        def step(k, _):
            load_j(side, k).wait()
            rows = pl.ds(pl.multiple_of(k * CHUNK, CHUNK), CHUNK)
            high, low = split2(j_buf[side, rows])
            lead = high_t[:, rows]
            value = mm(lead, low) + mm(low_t[:, rows], high) + mm(lead, high)
            for s in range(3):
                for t in range(SIDE):
                    at = pl.ds(pl.multiple_of(sides[side] + 128 * t, 128), 128)
                    y_ref[s, at] += value[128 * s : 128 * (s + 1), 128 * t : 128 * (t + 1)]
            return 0

        lax.fori_loop(0, chunks, step, 0)

    links.meet()
    stage = {3: share_core(links, 3, y_ref, r0, sems[0])}
    project(0)
    for s in range(3):
        stage[s] = share_core(links, s, y_ref, r0, sems[0])
    stage[3] = share_line(links, 3, stage[3], y_ref, r0, z0, r1, sems[1])
    project(1)
    stage[3] = share_plane(links, 3, stage[3], z0, r1, z1, r2, sems[2])
    for s in range(3):
        stage[s] = share_line(links, s, stage[s], y_ref, r0, z0, r1, sems[1])
    stage[3] = spread_plane(links, 3, stage[3], z1, r2, out_ref, sems[3])
    for s in range(3):
        stage[s] = share_plane(links, s, stage[s], z0, r1, z1, r2, sems[2])
    last = []
    stage[3], gram = spread_line(links, 3, stage[3], out_ref, sems[4], sems[5])
    for s in range(3):
        stage[s] = spread_plane(links, s, stage[s], z1, r2, out_ref, sems[3])
    gram += spread_core(links, 3, stage[3], out_ref, sems[5])
    for s in range(3):
        stage[s], own = spread_line(links, s, stage[s], out_ref, sems[4], sems[5])
        last += own
    for copy in gram:
        copy.wait_recv()
    b_ref[...] = gram_part(out_ref, scale)
    for s in range(3):
        last += spread_core(links, s, stage[s], out_ref, sems[5])
    hess = half_square(out_ref, sides[1])
    for copy in last:
        copy.wait_recv()
    b_ref[...] += (hess + half_square(out_ref, sides[0])) * scale
    for copy in links.sent:
        copy.wait_send()


def summed_products(basis, new_vectors, jacobian, scale):
    f32, bf16, dma = jnp.float32, jnp.bfloat16, pltpu.SemaphoreType.DMA
    rows = basis.shape[0]
    joint = basis.shape[1] + new_vectors.shape[1]
    sems = []
    for count in (4, 3, len(PLANE), len(PLANE), 3, 4):
        sems += [dma((STREAMS, count))] * 2
    return pl.pallas_call(
        functools.partial(gram_and_project, scale),
        out_shape=jax.ShapeDtypeStruct((joint, joint), f32),
        in_specs=[pl.BlockSpec(memory_space=pltpu.HBM)] * 3,
        out_specs=pl.BlockSpec(memory_space=pltpu.VMEM),
        scratch_shapes=[
            pltpu.VMEM((STREAMS, ROWS, 128), f32),
            pltpu.VMEM((rows, joint), f32),
            pltpu.VMEM((2, rows, HALF), f32),
            pltpu.VMEM((joint, rows), bf16),
            pltpu.VMEM((joint, rows), bf16),
            pltpu.VMEM((joint, 2 * joint), f32),
            pltpu.VMEM((STREAMS, ROWS, 128), f32),
            pltpu.VMEM((STREAMS, SIDE, PART, 128), f32),
            pltpu.VMEM((STREAMS, HALF, 128), f32),
            pltpu.VMEM((STREAMS, 3, PART, 128), f32),
            pltpu.VMEM((STREAMS, PART, 128), f32),
            pltpu.VMEM((STREAMS, len(PLANE), PIECE, 128), f32),
            dma((2, rows // CHUNK)),
            dma((2, rows // CHUNK)),
        ]
        + sems,
        compiler_params=pltpu.CompilerParams(
            collective_id=0, has_side_effects=True, vmem_limit_bytes=VMEM_LIMIT
        ),
        name="summed_products",
    )(basis, new_vectors, jacobian)


LEAF = 32
PIECES = 8


def eliminate(panel, columns):
    tiles = LEAF // 8
    lanes = len(panel) // tiles
    sub = lax.broadcasted_iota(jnp.int32, (8, 128), 0)
    factor = [jnp.zeros((8, 128), jnp.float32) for _ in range(tiles)]
    for j in range(LEAF):
        home, row = j // 8, j % 8
        pivot = jnp.broadcast_to(columns[j, home][row : row + 1], (8, 128))
        root = lax.rsqrt(pivot)
        inverse = root * root
        factor[home] = jnp.where(sub == row, root, factor[home])
        if j + 1 == LEAF:
            break
        mult = {}
        for t in range(home, tiles):
            value = columns[j, t] * inverse
            if t == home:
                value = jnp.where(sub > row, value, 0.0)
            mult[t] = value
        for k in range(j + 1, LEAF):
            spread = jnp.broadcast_to(columns[j, k // 8][k % 8 : k % 8 + 1], (8, 128))
            for t in range(k // 8, tiles):
                if k == j + 1:
                    columns[k, t] = columns[k, t] - (columns[j, t] * spread) * inverse
                else:
                    columns[k, t] = columns[k, t] - mult[t] * spread
        for c in range(lanes):
            spread = jnp.broadcast_to(panel[home, c][row : row + 1], (8, 128))
            for t in range(home, tiles):
                panel[t, c] = panel[t, c] - mult[t] * spread
    return jnp.concatenate(
        [jnp.concatenate([panel[t, c] * factor[t] for c in range(lanes)], axis=1) for t in range(tiles)], axis=0
    )


def factor_inverse(a, x):
    width = a.shape[0]
    tiles, lanes = LEAF // 8, width // 128
    lane = lax.broadcasted_iota(jnp.int32, (8, 128), 1)
    sub = lax.broadcasted_iota(jnp.int32, (8, 128), 0)
    ahead = a[0:LEAF]
    for first in range(0, width, LEAF):
        block = first // 128
        after = first + LEAF
        panel, columns = {}, {}
        for t in range(tiles):
            for c in range(lanes):
                value = ahead[8 * t : 8 * t + 8, 128 * c : 128 * (c + 1)]
                if c == block:
                    for k in range(min(LEAF, 8 * (t + 1))):
                        at = first % 128 + k
                        columns[k, t] = jnp.broadcast_to(value[:, at : at + 1], (8, 128))
                    place = lane - first % 128
                    unit = jnp.where(place == sub + 8 * t, 1.0, 0.0)
                    value = jnp.where((place >= 0) & (place < LEAF), unit, value)
                panel[t, c] = value
        rows = eliminate(panel, columns)
        column = lax.broadcasted_iota(jnp.int32, (LEAF, width), 1)
        x[first:after] = jnp.where(column < after, rows, 0.0)
        if after == width:
            break
        none = jnp.zeros((LEAF, width), jnp.bfloat16)
        pick = lambda parts, order: jnp.concatenate(
            [parts[i] for i in order] + [none[:, : parts[0].shape[1]]] * (PIECES - len(order)), axis=0
        )
        parts = split3(rows)
        right = pick(parts, (0, 1, 0, 2, 0, 1))
        low = 128 * (after // 128)
        left = pick(tuple(part[:, low:] for part in parts), (0, 0, 1, 0, 2, 1)).T

        def rest(start, stop):
            held = a[start:stop]
            place = lax.broadcasted_iota(jnp.int32, held.shape, 1)
            held = jnp.where((place >= first) & (place < after), 0.0, held)
            return held - mm(left[start - low : stop - low], right)

        ahead = rest(after, after + LEAF)
        if after + LEAF < width:
            a[after + LEAF : width] = rest(after + LEAF, width)


OUT_CHUNK = 512


def merge_kernel(b_ref, v_ref, w_ref, out_ref, a, x, s_buf, o_buf, in_sems, out_sems):
    width = v_ref.shape[1]
    joint = s_buf.shape[1]
    loads = (
        pltpu.make_async_copy(v_ref, s_buf.at[:, pl.ds(0, width)], in_sems.at[0]),
        pltpu.make_async_copy(w_ref, s_buf.at[:, pl.ds(width, joint - width)], in_sems.at[1]),
    )
    for copy in loads:
        copy.start()
    a[...] = b_ref[...]
    factor_inverse(a, x)
    for copy in loads:
        copy.wait()
    high, low = split2(x[...].T)
    edge = 256
    both = jnp.concatenate([high[:, edge:], low[:, edge:]], axis=1)

    def store(k):
        rows = pl.ds(pl.multiple_of(k * OUT_CHUNK, OUT_CHUNK), OUT_CHUNK)
        return pltpu.make_async_copy(o_buf.at[rows], out_ref.at[rows], out_sems.at[k])

    def step(k, _):
        rows = pl.ds(pl.multiple_of(k * OUT_CHUNK, OUT_CHUNK), OUT_CHUNK)
        lead, trail = split2(s_buf[rows])
        first, second = lead[:, :edge], trail[:, :edge]
        o_buf[rows, 0:edge] = (
            mm(first, low[:edge, :edge]) + mm(second, high[:edge, :edge]) + mm(first, high[:edge, :edge])
        )
        wide = mm(lead, both)
        o_buf[rows, edge:joint] = wide[:, : joint - edge] + (wide[:, joint - edge :] + mm(trail, high[:, edge:]))
        store(k).start()
        return 0

    chunks = s_buf.shape[0] // OUT_CHUNK
    lax.fori_loop(0, chunks, step, 0)
    for k in range(chunks):
        store(k).wait()


def merge(matrix, basis, new_vectors):
    f32, dma = jnp.float32, pltpu.SemaphoreType.DMA
    rows = basis.shape[0]
    joint = basis.shape[1] + new_vectors.shape[1]
    hbm = pl.BlockSpec(memory_space=pltpu.HBM)
    return pl.pallas_call(
        merge_kernel,
        out_shape=jax.ShapeDtypeStruct((rows, joint), f32),
        in_specs=[pl.BlockSpec(memory_space=pltpu.VMEM), hbm, hbm],
        out_specs=hbm,
        scratch_shapes=[
            pltpu.VMEM((joint, joint), f32),
            pltpu.VMEM((joint, joint), f32),
            pltpu.VMEM((rows, joint), f32),
            pltpu.VMEM((rows, joint), f32),
            dma((2,)),
            dma((rows // OUT_CHUNK,)),
        ],
        compiler_params=pltpu.CompilerParams(vmem_limit_bytes=VMEM_LIMIT),
        name="merge",
    )(matrix, basis, new_vectors)


def local(basis, new_vectors, jacobian):
    total = basis.shape[0] * lax.axis_size("rows") * lax.axis_size("cols")
    scale = 1.0 / total
    matrix = summed_products(basis, new_vectors, jacobian, scale)
    return merge(matrix, basis, new_vectors)


def solution(mesh):
    placed = (P(("rows", "cols"), None), P(("rows", "cols"), None), P(("rows", "cols"), None))
    return jax.shard_map(
        local, mesh=mesh, in_specs=placed, out_specs=P(("rows", "cols"), None), check_vma=False
    )
```

```python
import functools

import jax
import jax.numpy as jnp
from jax import lax
from jax.experimental import pallas as pl
from jax.experimental.pallas import tpu as pltpu
from jax.sharding import PartitionSpec as P

SIDE = 4
STREAMS = 4
AXIS = (0, 1, 2, 0)
OFFSETS = (2, 1, 3, 0)
PLANE = sorted(
    [(b, c) for b in range(SIDE) for c in range(SIDE) if b or c],
    key=lambda at: -(min(at[0], SIDE - at[0]) + min(at[1], SIDE - at[1])),
)
ROWS = 1024
VMEM_LIMIT = 55_000_000
HALF = ROWS // 2
PART = HALF // SIDE
PIECE = PART // SIDE**2
ORDER = (3, 0, 1, 2)


class Links:
    def __init__(self):
        row, col = lax.axis_index("rows"), lax.axis_index("cols")
        self.core = lax.rem(row, 2)
        self.place = (lax.div(row, 2 * SIDE), col, lax.rem(lax.div(row, 2), SIDE))
        self.partner = self.device(self.place, 1 - self.core)
        self.sent = []

    def device(self, coords, which):
        return (coords[0] * (2 * SIDE) + coords[2] * 2 + which, coords[1])

    def moved(self, axes, offsets):
        coords = list(self.place)
        for axis, offset in zip(axes, offsets):
            coords[axis] = lax.rem(self.place[axis] + offset, SIDE)
        return coords

    def greet(self):
        barrier = pltpu.get_barrier_semaphore()
        others = [self.partner]
        for axis in range(3):
            others += [self.device(self.moved((axis,), (offset,)), self.core) for offset in OFFSETS[:3]]
        for axes in ((1, 2), (0, 2), (0, 1)):
            others += [self.device(self.moved(axes, at), self.core) for at in PLANE if at[0] and at[1]]
        for other in others:
            pl.semaphore_signal(barrier, inc=1, device_id=other, device_id_type=pl.DeviceIdType.MESH)
        self.greeted = (barrier, len(others))

    def meet(self):
        pl.semaphore_wait(*self.greeted)

    def send(self, src, dst, sems, at, target):
        copy = pltpu.make_async_remote_copy(
            src_ref=src,
            dst_ref=dst,
            send_sem=sems[0].at[at],
            recv_sem=sems[1].at[at],
            device_id=target,
            device_id_type=pl.DeviceIdType.MESH,
        )
        copy.start()
        self.sent.append(copy)
        return copy


def plane_of(s):
    return tuple(axis for axis in range(3) if axis != AXIS[s])


def share_core(links, s, y_ref, r0, sems):
    copies = []
    for slot, offset in enumerate(OFFSETS):
        at = links.moved((AXIS[s],), (offset,))[AXIS[s]] * PART
        rows = pl.ds(pl.multiple_of((1 - links.core) * HALF + at, PART), PART)
        keep = pl.ds(pl.multiple_of(at, PART), PART)
        copies.append(links.send(y_ref.at[s, rows], r0.at[s, keep], sems, (s, slot), links.partner))
    return copies


def share_line(links, s, waits, y_ref, r0, z0, r1, sems):
    copies = []
    for slot, offset in enumerate(OFFSETS):
        coords = links.moved((AXIS[s],), (offset,))
        at = coords[AXIS[s]] * PART
        rows = pl.ds(pl.multiple_of(links.core * HALF + at, PART), PART)
        keep = pl.ds(pl.multiple_of(at, PART), PART)
        waits[slot].wait_recv()
        z0[s, slot] = y_ref[s, rows] + r0[s, keep]
        if offset:
            copies.append(links.send(z0.at[s, slot], r1.at[s, slot], sems, (s, slot), links.device(coords, links.core)))
    return copies


def share_plane(links, s, waits, z0, r1, z1, r2, sems):
    for copy in waits:
        copy.wait_recv()
    z1[s] = (z0[s, 3] + r1[s, 0]) + (r1[s, 1] + r1[s, 2])
    copies = []
    axes = plane_of(s)
    for slot, offsets in enumerate(PLANE):
        coords = links.moved(axes, offsets)
        at = pl.multiple_of((coords[axes[0]] * SIDE + coords[axes[1]]) * PIECE, PIECE)
        copies.append(
            links.send(z1.at[s, pl.ds(at, PIECE)], r2.at[s, slot], sems, (s, slot), links.device(coords, links.core))
        )
    return copies


def spread_plane(links, s, waits, z1, r2, out_ref, sems):
    for copy in waits:
        copy.wait_recv()
    axes = plane_of(s)
    at = (links.place[axes[0]] * SIDE + links.place[axes[1]]) * PIECE
    parts = [z1[s, pl.ds(pl.multiple_of(at, PIECE), PIECE)]] + [r2[s, slot] for slot in range(len(PLANE))]
    while len(parts) > 1:
        parts = [left + right for left, right in zip(parts[::2], parts[1::2])]
    rows = pl.ds(pl.multiple_of(links.core * HALF + links.place[AXIS[s]] * PART + at, PIECE), PIECE)
    out_ref[s, rows] = parts[0]
    return [
        links.send(
            out_ref.at[s, rows],
            out_ref.at[s, rows],
            sems,
            (s, slot),
            links.device(links.moved(axes, offsets), links.core),
        )
        for slot, offsets in enumerate(PLANE)
    ]


def spread_line(links, s, waits, out_ref, sems, core_sems):
    for copy in waits:
        copy.wait_recv()
    rows = pl.ds(pl.multiple_of(links.core * HALF + links.place[AXIS[s]] * PART, PART), PART)
    block = out_ref.at[s, rows]
    copies = [
        links.send(block, block, sems, (s, slot), links.device(links.moved((AXIS[s],), (offset,)), links.core))
        for slot, offset in enumerate(OFFSETS[:3])
    ]
    return copies, [links.send(block, block, core_sems, (s, 3), links.partner)]


def spread_core(links, s, waits, out_ref, core_sems):
    copies = []
    for slot in (1, 2, 0):
        waits[slot].wait_recv()
        at = links.moved((AXIS[s],), (SIDE - OFFSETS[slot],))[AXIS[s]] * PART
        block = out_ref.at[s, pl.ds(pl.multiple_of(links.core * HALF + at, PART), PART)]
        copies.append(links.send(block, block, core_sems, (s, slot), links.partner))
    return copies


def split3(value):
    high = value.astype(jnp.bfloat16)
    rest = value - high.astype(jnp.float32)
    middle = rest.astype(jnp.bfloat16)
    low = (rest - middle.astype(jnp.float32)).astype(jnp.bfloat16)
    return high, middle, low


def split2(value):
    high = value.astype(jnp.bfloat16)
    return high, (value - high.astype(jnp.float32)).astype(jnp.bfloat16)


def mat(left, right, precision=lax.Precision.HIGHEST):
    return jnp.dot(left, right, precision=precision, preferred_element_type=jnp.float32)


def tmat(left, right, precision=lax.Precision.HIGHEST):
    return lax.dot_general(
        left,
        right,
        (((0,), (0,)), ((), ())),
        precision=precision,
        preferred_element_type=jnp.float32,
    )


def gram_part(y_ref, scale):
    cut = {}
    at = 0
    for i in range(3):
        for j in range(i + 1):
            cut[i, j] = y_ref[3, at : at + 128] * scale
            at += 128
    s_vv = jnp.concatenate(
        [jnp.concatenate([cut[0, 0], cut[1, 0].T], axis=1), jnp.concatenate([cut[1, 0], cut[1, 1]], axis=1)], axis=0
    )
    s_vw = jnp.concatenate([cut[2, 0].T, cut[2, 1].T], axis=0)
    summed = s_vw + (s_vw - mat(s_vv, s_vw))
    cross = tmat(summed, s_vw)
    last = cut[2, 2] - cross - cross.T + tmat(summed, mat(s_vv, summed) + summed)
    ident = jnp.where(
        lax.broadcasted_iota(jnp.int32, (256, 256), 0) == lax.broadcasted_iota(jnp.int32, (256, 256), 1), 1.0, 0.0
    ).astype(jnp.float32)
    top = jnp.concatenate([ident, summed], axis=1)
    low = jnp.concatenate([summed.T, last], axis=1)
    return jnp.concatenate([top, low], axis=0)


def nt(left, right):
    return lax.dot_general(left, right, (((1,), (1,)), ((), ())), preferred_element_type=jnp.float32)


def half_square(y_ref, start):
    total = None
    for pair in range(0, HALF, 256):
        blocks = []
        for t in (pair, pair + 128):
            rows = pl.ds(pl.multiple_of(start + t, 128), 128)
            blocks.append(jnp.concatenate([y_ref[s, rows] for s in range(3)], axis=0))
        high, low = split2(jnp.concatenate(blocks, axis=1))
        value = nt(high, low) + nt(low, high) + nt(high, high)
        total = value if total is None else total + value
    return total


CHUNK = 512


def mm(left, right):
    return jnp.dot(left, right, preferred_element_type=jnp.float32)


def gram_and_project(scale, v_ref, w_ref, j_ref, b_ref, out_ref, s_buf, j_buf, high_t, low_t, g_acc, y_ref, z0, r0, r1, z1, r2, in_s, in_j, *sems):
    sems = [sems[i : i + 2] for i in range(0, 12, 2)]
    links = Links()
    links.greet()
    width, block = v_ref.shape[1], w_ref.shape[1]
    joint = width + block
    chunks = v_ref.shape[0] // CHUNK
    sides = [pl.multiple_of(which * HALF, HALF) for which in (1 - links.core, links.core)]

    def load_s(k):
        rows = pl.ds(pl.multiple_of(k * CHUNK, CHUNK), CHUNK)
        return (
            pltpu.make_async_copy(v_ref.at[rows], s_buf.at[rows, pl.ds(0, width)], in_s.at[0, k]),
            pltpu.make_async_copy(w_ref.at[rows], s_buf.at[rows, pl.ds(width, block)], in_s.at[1, k]),
        )

    def load_j(side, k):
        rows = pl.ds(pl.multiple_of(k * CHUNK, CHUNK), CHUNK)
        return pltpu.make_async_copy(j_ref.at[rows, pl.ds(sides[side], HALF)], j_buf.at[side, rows], in_j.at[side, k])

    for k in range(chunks):
        for copy in load_s(k):
            copy.start()
    for side in range(2):
        for k in range(chunks):
            load_j(side, k).start()
    g_acc[...] = jnp.zeros_like(g_acc)
    y_ref[...] = jnp.zeros_like(y_ref)

    def gram_step(k, _):
        for copy in load_s(k):
            copy.wait()
        rows = pl.ds(pl.multiple_of(k * CHUNK, CHUNK), CHUNK)
        value = s_buf[rows]
        flipped = split2(value.T)
        high_t[:, rows], low_t[:, rows] = flipped
        g_acc[...] += mm(flipped[0], jnp.concatenate(split2(value), axis=1))
        return 0

    lax.fori_loop(0, chunks, gram_step, 0)
    at = 0
    for i in range(3):
        for j in range(i + 1):
            tile = g_acc[128 * i : 128 * (i + 1), 128 * j : 128 * (j + 1)]
            mixed = g_acc[128 * i : 128 * (i + 1), joint + 128 * j : joint + 128 * (j + 1)]
            other = g_acc[128 * j : 128 * (j + 1), joint + 128 * i : joint + 128 * (i + 1)]
            y_ref[3, at : at + 128] = tile + (mixed + other.T)
            at += 128

    def project(side):
        def step(k, _):
            load_j(side, k).wait()
            rows = pl.ds(pl.multiple_of(k * CHUNK, CHUNK), CHUNK)
            high, low = split2(j_buf[side, rows])
            lead = high_t[:, rows]
            value = mm(lead, low) + mm(low_t[:, rows], high) + mm(lead, high)
            for s in range(3):
                for t in range(SIDE):
                    at = pl.ds(pl.multiple_of(sides[side] + 128 * t, 128), 128)
                    y_ref[s, at] += value[128 * s : 128 * (s + 1), 128 * t : 128 * (t + 1)]
            return 0

        lax.fori_loop(0, chunks, step, 0)

    links.meet()
    stage = {3: share_core(links, 3, y_ref, r0, sems[0])}
    project(0)
    for s in range(3):
        stage[s] = share_core(links, s, y_ref, r0, sems[0])
    stage[3] = share_line(links, 3, stage[3], y_ref, r0, z0, r1, sems[1])
    project(1)
    stage[3] = share_plane(links, 3, stage[3], z0, r1, z1, r2, sems[2])
    for s in range(3):
        stage[s] = share_line(links, s, stage[s], y_ref, r0, z0, r1, sems[1])
    stage[3] = spread_plane(links, 3, stage[3], z1, r2, out_ref, sems[3])
    for s in range(3):
        stage[s] = share_plane(links, s, stage[s], z0, r1, z1, r2, sems[2])
    last = []
    stage[3], gram = spread_line(links, 3, stage[3], out_ref, sems[4], sems[5])
    for s in range(3):
        stage[s] = spread_plane(links, s, stage[s], z1, r2, out_ref, sems[3])
    gram += spread_core(links, 3, stage[3], out_ref, sems[5])
    for s in range(3):
        stage[s], own = spread_line(links, s, stage[s], out_ref, sems[4], sems[5])
        last += own
    for copy in gram:
        copy.wait_recv()
    b_ref[...] = gram_part(out_ref, scale)
    for s in range(3):
        last += spread_core(links, s, stage[s], out_ref, sems[5])
    hess = half_square(out_ref, sides[1])
    for copy in last:
        copy.wait_recv()
    b_ref[...] += (hess + half_square(out_ref, sides[0])) * scale
    for copy in links.sent:
        copy.wait_send()


def summed_products(basis, new_vectors, jacobian, scale):
    f32, bf16, dma = jnp.float32, jnp.bfloat16, pltpu.SemaphoreType.DMA
    rows = basis.shape[0]
    joint = basis.shape[1] + new_vectors.shape[1]
    sems = []
    for count in (4, 3, len(PLANE), len(PLANE), 3, 4):
        sems += [dma((STREAMS, count))] * 2
    return pl.pallas_call(
        functools.partial(gram_and_project, scale),
        out_shape=jax.ShapeDtypeStruct((joint, joint), f32),
        in_specs=[pl.BlockSpec(memory_space=pltpu.HBM)] * 3,
        out_specs=pl.BlockSpec(memory_space=pltpu.VMEM),
        scratch_shapes=[
            pltpu.VMEM((STREAMS, ROWS, 128), f32),
            pltpu.VMEM((rows, joint), f32),
            pltpu.VMEM((2, rows, HALF), f32),
            pltpu.VMEM((joint, rows), bf16),
            pltpu.VMEM((joint, rows), bf16),
            pltpu.VMEM((joint, 2 * joint), f32),
            pltpu.VMEM((STREAMS, ROWS, 128), f32),
            pltpu.VMEM((STREAMS, SIDE, PART, 128), f32),
            pltpu.VMEM((STREAMS, HALF, 128), f32),
            pltpu.VMEM((STREAMS, 3, PART, 128), f32),
            pltpu.VMEM((STREAMS, PART, 128), f32),
            pltpu.VMEM((STREAMS, len(PLANE), PIECE, 128), f32),
            dma((2, rows // CHUNK)),
            dma((2, rows // CHUNK)),
        ]
        + sems,
        compiler_params=pltpu.CompilerParams(
            collective_id=0, has_side_effects=True, vmem_limit_bytes=VMEM_LIMIT
        ),
        name="summed_products",
    )(basis, new_vectors, jacobian)


LEAF = 32
PIECES = 8


def eliminate(panel, columns):
    tiles = LEAF // 8
    lanes = len(panel) // tiles
    sub = lax.broadcasted_iota(jnp.int32, (8, 128), 0)
    factor = [jnp.zeros((8, 128), jnp.float32) for _ in range(tiles)]
    for j in range(LEAF):
        home, row = j // 8, j % 8
        pivot = jnp.broadcast_to(columns[j, home][row : row + 1], (8, 128))
        root = lax.rsqrt(pivot)
        inverse = root * root
        factor[home] = jnp.where(sub == row, root, factor[home])
        if j + 1 == LEAF:
            break
        mult = {}
        for t in range(home, tiles):
            value = columns[j, t] * inverse
            if t == home:
                value = jnp.where(sub > row, value, 0.0)
            mult[t] = value
        for k in range(j + 1, LEAF):
            spread = jnp.broadcast_to(columns[j, k // 8][k % 8 : k % 8 + 1], (8, 128))
            for t in range(k // 8, tiles):
                columns[k, t] = columns[k, t] - mult[t] * spread
        for c in range(lanes):
            spread = jnp.broadcast_to(panel[home, c][row : row + 1], (8, 128))
            for t in range(home, tiles):
                panel[t, c] = panel[t, c] - mult[t] * spread
    return jnp.concatenate(
        [jnp.concatenate([panel[t, c] * factor[t] for c in range(lanes)], axis=1) for t in range(tiles)], axis=0
    )


def factor_inverse(a, x):
    width = a.shape[0]
    tiles, lanes = LEAF // 8, width // 128
    lane = lax.broadcasted_iota(jnp.int32, (8, 128), 1)
    sub = lax.broadcasted_iota(jnp.int32, (8, 128), 0)
    ahead = a[0:LEAF]
    for first in range(0, width, LEAF):
        block = first // 128
        after = first + LEAF
        panel, columns = {}, {}
        for t in range(tiles):
            for c in range(lanes):
                value = ahead[8 * t : 8 * t + 8, 128 * c : 128 * (c + 1)]
                if c == block:
                    for k in range(min(LEAF, 8 * (t + 1))):
                        at = first % 128 + k
                        columns[k, t] = jnp.broadcast_to(value[:, at : at + 1], (8, 128))
                    place = lane - first % 128
                    unit = jnp.where(place == sub + 8 * t, 1.0, 0.0)
                    value = jnp.where((place >= 0) & (place < LEAF), unit, value)
                panel[t, c] = value
        rows = eliminate(panel, columns)
        column = lax.broadcasted_iota(jnp.int32, (LEAF, width), 1)
        x[first:after] = jnp.where(column < after, rows, 0.0)
        if after == width:
            break
        none = jnp.zeros((LEAF, width), jnp.bfloat16)
        pick = lambda parts, order: jnp.concatenate(
            [parts[i] for i in order] + [none[:, : parts[0].shape[1]]] * (PIECES - len(order)), axis=0
        )
        parts = split3(rows)
        right = pick(parts, (0, 1, 0, 2, 0, 1))
        low = 128 * (after // 128)
        left = pick(tuple(part[:, low:] for part in parts), (0, 0, 1, 0, 2, 1)).T

        def rest(start, stop):
            held = a[start:stop]
            place = lax.broadcasted_iota(jnp.int32, held.shape, 1)
            held = jnp.where((place >= first) & (place < after), 0.0, held)
            return held - mm(left[start - low : stop - low], right)

        ahead = rest(after, after + LEAF)
        if after + LEAF < width:
            a[after + LEAF : width] = rest(after + LEAF, width)


OUT_CHUNK = 512


def merge_kernel(b_ref, v_ref, w_ref, out_ref, a, x, s_buf, o_buf, in_sems, out_sems):
    width = v_ref.shape[1]
    joint = s_buf.shape[1]
    loads = (
        pltpu.make_async_copy(v_ref, s_buf.at[:, pl.ds(0, width)], in_sems.at[0]),
        pltpu.make_async_copy(w_ref, s_buf.at[:, pl.ds(width, joint - width)], in_sems.at[1]),
    )
    for copy in loads:
        copy.start()
    a[...] = b_ref[...]
    factor_inverse(a, x)
    for copy in loads:
        copy.wait()
    high, low = split2(x[...].T)
    edge = 256
    both = jnp.concatenate([high[:, edge:], low[:, edge:]], axis=1)

    def store(k):
        rows = pl.ds(pl.multiple_of(k * OUT_CHUNK, OUT_CHUNK), OUT_CHUNK)
        return pltpu.make_async_copy(o_buf.at[rows], out_ref.at[rows], out_sems.at[k])

    def step(k, _):
        rows = pl.ds(pl.multiple_of(k * OUT_CHUNK, OUT_CHUNK), OUT_CHUNK)
        lead, trail = split2(s_buf[rows])
        first, second = lead[:, :edge], trail[:, :edge]
        o_buf[rows, 0:edge] = (
            mm(first, low[:edge, :edge]) + mm(second, high[:edge, :edge]) + mm(first, high[:edge, :edge])
        )
        wide = mm(lead, both)
        o_buf[rows, edge:joint] = wide[:, : joint - edge] + (wide[:, joint - edge :] + mm(trail, high[:, edge:]))
        store(k).start()
        return 0

    chunks = s_buf.shape[0] // OUT_CHUNK
    lax.fori_loop(0, chunks, step, 0)
    for k in range(chunks):
        store(k).wait()


def merge(matrix, basis, new_vectors):
    f32, dma = jnp.float32, pltpu.SemaphoreType.DMA
    rows = basis.shape[0]
    joint = basis.shape[1] + new_vectors.shape[1]
    hbm = pl.BlockSpec(memory_space=pltpu.HBM)
    return pl.pallas_call(
        merge_kernel,
        out_shape=jax.ShapeDtypeStruct((rows, joint), f32),
        in_specs=[pl.BlockSpec(memory_space=pltpu.VMEM), hbm, hbm],
        out_specs=hbm,
        scratch_shapes=[
            pltpu.VMEM((joint, joint), f32),
            pltpu.VMEM((joint, joint), f32),
            pltpu.VMEM((rows, joint), f32),
            pltpu.VMEM((rows, joint), f32),
            dma((2,)),
            dma((rows // OUT_CHUNK,)),
        ],
        compiler_params=pltpu.CompilerParams(
            vmem_limit_bytes=VMEM_LIMIT
        ),
        name="merge",
    )(matrix, basis, new_vectors)


def local(basis, new_vectors, jacobian):
    total = basis.shape[0] * lax.axis_size("rows") * lax.axis_size("cols")
    scale = 1.0 / total
    matrix = summed_products(basis, new_vectors, jacobian, scale)
    return merge(matrix, basis, new_vectors)


def solution(mesh):
    placed = (P(("rows", "cols"), None), P(("rows", "cols"), None), P(("rows", "cols"), None))
    return jax.shard_map(
        local, mesh=mesh, in_specs=placed, out_specs=P(("rows", "cols"), None), check_vma=False
    )
```
